32 devices in a mesh: blk: 4 (over x, core), uly: 8 (over z, y).
Axes of the slice: x: 2, y: 2, z: 4, core: 2. Of those that a mesh axis runs over, the one named last changes fastest.
Arguments:
- query: bfloat16 [4096, 4096], P(('blk', 'uly')), may hold values from -5 to 5
- key_input: bfloat16 [4096, 512], P(('blk', 'uly')), may hold values from -5 to 5
- value_input: bfloat16 [4096, 512], P(('blk', 'uly')), may hold values from -6 to 6
- output: bfloat16 [4096, 4096], P(('blk', 'uly')), may hold values from -6 to 6
- out_grad: bfloat16 [4096, 4096], P(('blk', 'uly')), may hold values from -6 to 6
Outputs:
- query_grad: bfloat16 [4096, 4096], P(('blk', 'uly'))
- key_gradient: bfloat16 [4096, 512], P(('blk', 'uly'))
- value_gradient: bfloat16 [4096, 512], P(('blk', 'uly'))
The draws below stay inside these ranges and needn't reach their ends.
All inputs are finite; a program needn't handle non-finite values.
Results may differ from the reference program's by a relative error of at most 0.009.
Values may be sent and summed in bfloat16 or wider, within the bound.
A program may use at most 64 MiB of HBM per device.

```python
import jax
import jax.numpy as jnp
from jax import lax

QUERY_HEADS = 32
KEY_VALUE_HEADS = 4
HEAD_SIZE = 128
WINDOW_KEYS = 1024
SEQUENCE_TOKENS = 4096


def draw_query(key, part):
    start_offset = jnp.clip(jax.random.normal(jax.random.fold_in(key, 1), (SEQUENCE_TOKENS, QUERY_HEADS * HEAD_SIZE), jnp.float32), -5.0, 5.0)
    return start_offset.astype(jnp.bfloat16)


def draw_key_input(key, part):
    start_offset = jnp.clip(jax.random.normal(jax.random.fold_in(key, 5), (SEQUENCE_TOKENS, KEY_VALUE_HEADS * HEAD_SIZE), jnp.float32), -5.0, 5.0)
    return start_offset.astype(jnp.bfloat16)


def block_scale(key, extent, pieces, least, top_value):
    loudness, own = 1.0, jax.random.fold_in(key, 6)
    for position, parts in pieces:
        heights = jnp.exp(jax.random.uniform(jax.random.fold_in(own, position), (parts,), jnp.float32, least / len(pieces), top_value / len(pieces)))
        loudness = loudness * jnp.repeat(heights, extent[position] // parts).reshape([-1 if axis == position else 1 for axis in range(len(extent))])
    return loudness


def gaussian(key, shape, scale, limit, cuts=(), kind=jnp.bfloat16):
    drawn = jax.random.normal(key, shape, jnp.float32) * scale
    if len(cuts) > 0:
        drawn = block_scale(key, shape, cuts, -0.22, 0.18) * drawn
    return jnp.clip(drawn, min=-limit, max=limit).astype(kind)


def setup_inputs(seed: int = 0) -> dict:
    streams_of = jax.random.split(jax.random.key(seed), 6)
    query = draw_query(jax.random.fold_in(streams_of[5], 71), 0)
    key_input = draw_key_input(jax.random.fold_in(streams_of[5], 71), 0)
    value_input = gaussian(streams_of[2], (SEQUENCE_TOKENS, KEY_VALUE_HEADS * HEAD_SIZE), 1.0, 6.0, ((0, 32),))
    output = gaussian(streams_of[3], (SEQUENCE_TOKENS, QUERY_HEADS * HEAD_SIZE), 1.0, 6.0, ((0, 32),))
    out_grad = gaussian(streams_of[4], (SEQUENCE_TOKENS, QUERY_HEADS * HEAD_SIZE), 1.0, 6.0, ((0, 32),))
    return dict(query=query, key_input=key_input, value_input=value_input, output=output, out_grad=out_grad)


def reference(query, key_input, value_input, output, out_grad):
    scaling = HEAD_SIZE ** -0.5
    group_width = QUERY_HEADS // KEY_VALUE_HEADS
    block = min(512, SEQUENCE_TOKENS)
    block_count = SEQUENCE_TOKENS // block
    span = WINDOW_KEYS + block
    highest = lax.Precision.HIGHEST
    query_heads = query.reshape(SEQUENCE_TOKENS, QUERY_HEADS, HEAD_SIZE).transpose(1, 0, 2)
    output_heads = output.reshape(SEQUENCE_TOKENS, QUERY_HEADS, HEAD_SIZE).transpose(1, 0, 2)
    grad_heads = out_grad.reshape(SEQUENCE_TOKENS, QUERY_HEADS, HEAD_SIZE).transpose(1, 0, 2)
    key_head_rows = jnp.pad(key_input.reshape(SEQUENCE_TOKENS, KEY_VALUE_HEADS, HEAD_SIZE).transpose(1, 0, 2), ((0, 0), (WINDOW_KEYS, 0), (0, 0)))
    value_head_rows = jnp.pad(value_input.reshape(SEQUENCE_TOKENS, KEY_VALUE_HEADS, HEAD_SIZE).transpose(1, 0, 2), ((0, 0), (WINDOW_KEYS, 0), (0, 0)))
    offsets = jnp.arange(block, dtype=jnp.int32)[:, None]
    columns = jnp.arange(span, dtype=jnp.int32)[None, :]
    relative = columns - offsets
    inside = (relative >= 1) & (relative <= WINDOW_KEYS)

    def group_member_count(group):
        key_pad = key_head_rows[group].astype(jnp.float32)
        value_pad = value_head_rows[group].astype(jnp.float32)

        def per_head(carry, member):
            key_acc, value_acc = carry
            head = group * group_width + member
            query_wide = query_heads[head].astype(jnp.float32)
            grad_wide = grad_heads[head].astype(jnp.float32)
            row_dot = jnp.sum(output_heads[head].astype(jnp.float32) * grad_wide, axis=1)

            def per_block(inner, index):
                key_acc, value_acc = inner
                start = (index * block).astype(jnp.int32)
                query_block = lax.dynamic_slice_in_dim(query_wide, start, block, 0)
                grad_block = lax.dynamic_slice_in_dim(grad_wide, start, block, 0)
                dot_block = lax.dynamic_slice_in_dim(row_dot, start, block, 0)
                key_block = lax.dynamic_slice_in_dim(key_pad, start, span, 0)
                value_block = lax.dynamic_slice_in_dim(value_pad, start, span, 0)
                visible = inside & (start - WINDOW_KEYS + columns >= 0)
                scores = jnp.dot(query_block, key_block.T, precision=highest) * scaling
                masked = jnp.where(visible, scores, -1e30)
                row_max = jnp.max(masked, axis=1)
                row_sum = jnp.sum(jnp.where(visible, jnp.exp(masked - row_max[:, None]), 0.0), axis=1)
                log_total = row_max + jnp.log(row_sum)
                weights = jnp.where(visible, jnp.exp(masked - log_total[:, None]), 0.0)
                weights_low = weights.astype(jnp.bfloat16).astype(jnp.float32)
                weight_grad = jnp.dot(grad_block, value_block.T, precision=highest)
                score_grad = (weights * (weight_grad - dot_block[:, None]) * scaling).astype(jnp.bfloat16)
                score_wide = score_grad.astype(jnp.float32)
                query_portion = jnp.dot(score_wide, key_block, precision=highest)
                key_portion = jnp.dot(score_wide.T, query_block, precision=highest)
                value_portion = jnp.dot(weights_low.T, grad_block, precision=highest)
                key_acc = lax.dynamic_update_slice_in_dim(
                    key_acc, lax.dynamic_slice_in_dim(key_acc, start, span, 0) + key_portion, start, 0)
                value_acc = lax.dynamic_update_slice_in_dim(
                    value_acc, lax.dynamic_slice_in_dim(value_acc, start, span, 0) + value_portion, start, 0)
                return (key_acc, value_acc), query_portion

            (key_acc, value_acc), query_parts = lax.scan(
                per_block, (key_acc, value_acc), jnp.arange(block_count, dtype=jnp.int32))
            return (key_acc, value_acc), query_parts.reshape(SEQUENCE_TOKENS, HEAD_SIZE).astype(jnp.bfloat16)

        zeros = jnp.zeros((SEQUENCE_TOKENS + WINDOW_KEYS, HEAD_SIZE), jnp.float32)
        (key_acc, value_acc), query_portion = lax.scan(
            per_head, (zeros, zeros), jnp.arange(group_width, dtype=jnp.int32))
        return query_portion, key_acc[WINDOW_KEYS:], value_acc[WINDOW_KEYS:]

    query_portion, key_portion, value_portion = lax.map(group_member_count, jnp.arange(KEY_VALUE_HEADS, dtype=jnp.int32))
    query_grad = query_portion.reshape(QUERY_HEADS, SEQUENCE_TOKENS, HEAD_SIZE).transpose(1, 0, 2).reshape(SEQUENCE_TOKENS, QUERY_HEADS * HEAD_SIZE)
    key_gradient = key_portion.transpose(1, 0, 2).reshape(SEQUENCE_TOKENS, KEY_VALUE_HEADS * HEAD_SIZE).astype(jnp.bfloat16)
    value_gradient = value_portion.transpose(1, 0, 2).reshape(SEQUENCE_TOKENS, KEY_VALUE_HEADS * HEAD_SIZE).astype(jnp.bfloat16)
    return (query_grad, key_gradient, value_gradient)
```

```python
import functools
import math

import jax
import jax.numpy as jnp
from jax import lax
from jax.experimental import pallas as pl
from jax.experimental.pallas import tpu as pltpu
from jax.sharding import PartitionSpec as P

QUERY_HEADS = 32
KEY_VALUE_HEADS = 4
HEAD_SIZE = 128
WINDOW_KEYS = 1024
GROUP = QUERY_HEADS // KEY_VALUE_HEADS
PAIRS = GROUP // 2
MESH = pl.DeviceIdType.MESH
F32 = jnp.float32
BF16 = jnp.bfloat16
NT = (((1,), (1,)), ((), ()))
TN = (((0,), (0,)), ((), ()))


def kernel(
    rows, back, blks, ulys,
    q_hbm, k_hbm, v_hbm, o_hbm, g_hbm,
    dq_ref, dk_ref, dv_ref,
    q_ref, o_ref, g_ref, kv, acc_k, acc_v, own, pg_send, pg_recv, c_send, c_recv,
    load_sem, kv_sem, chain_ss, chain_rs, pair_ss, pair_rs, pgs, pgr, cgs, cgr,
):
    half = back // 2
    heads = KEY_VALUE_HEADS
    scaling = HEAD_SIZE ** (-0.5)
    total = blks * ulys
    me = lax.axis_index("blk") * ulys + lax.axis_index("uly")
    par = lax.rem(me, 2)
    partner = me + 1 - 2 * par
    up, down = me + 2, me - 2
    has_up, has_down = up < total, down >= 0

    def where_is(t):
        return (t // ulys, lax.rem(t, ulys))

    loads = [
        pltpu.make_async_copy(s, d, load_sem.at[i])
        for i, (s, d) in enumerate(((q_hbm, q_ref), (o_hbm, o_ref), (g_hbm, g_ref)))
    ]
    kv_loads = []
    for h in range(heads):
        for i, src in enumerate((k_hbm, v_hbm)):
            kv_loads.append(
                pltpu.make_async_copy(
                    src.at[:, h * HEAD_SIZE : (h + 1) * HEAD_SIZE], kv.at[h, back, i], kv_sem.at[h, i]
                )
            )
    for copy in kv_loads:
        copy.start()
    for copy in loads:
        copy.start()

    barrier = pltpu.get_barrier_semaphore()

    @pl.when(has_up)
    def _():
        pl.semaphore_signal(barrier, inc=1, device_id=where_is(up), device_id_type=MESH)

    @pl.when(has_down)
    def _():
        pl.semaphore_signal(barrier, inc=1, device_id=where_is(down), device_id_type=MESH)

    pl.semaphore_signal(barrier, inc=1, device_id=where_is(partner), device_id_type=MESH)
    pl.semaphore_wait(barrier, 1 + has_up.astype(jnp.int32) + has_down.astype(jnp.int32))

    def clear(s, carry):
        @pl.when(me - back + s < 0)
        def _():
            for h in range(heads):
                kv[h, s] = jnp.zeros((2, rows, HEAD_SIZE), BF16)

        return carry

    lax.fori_loop(0, back, clear, 0)

    def chain_copy(h, k):
        return pltpu.make_async_remote_copy(
            src_ref=kv.at[h, back - 2 * k],
            dst_ref=kv.at[h, back - 2 * k - 2],
            send_sem=chain_ss.at[h, k],
            recv_sem=chain_rs.at[h, k],
            device_id=where_is(up),
            device_id_type=MESH,
        )

    def pair_copy(h, k):
        return pltpu.make_async_remote_copy(
            src_ref=kv.at[h, back - 2 * k - 2 * par],
            dst_ref=kv.at[h, back - 1 - 2 * k],
            send_sem=pair_ss.at[h, k],
            recv_sem=pair_rs.at[h, k],
            device_id=where_is(partner),
            device_id_type=MESH,
        )

    def chain_out(k):
        return has_up & (me - 2 * k >= 0)

    def pair_out(k):
        return me - 2 * k - 2 * par >= 0

    def send_own(h):
        @pl.when(has_up)
        def _():
            chain_copy(h, 0).start()

        @pl.when(par == 0)
        def _():
            pair_copy(h, 0).start()

    def gather_step(h, k):
        @pl.when(me - 2 * k - 2 >= 0)
        def _():
            chain_copy(h, k).wait_recv()

            @pl.when(has_up & (k < half - 1))
            def _():
                chain_copy(h, k + 1).start()

            nxt = k + 1 - par

            @pl.when(nxt < half)
            def _():
                pair_copy(h, nxt).start()

    def gather_finish(h, k):
        @pl.when(me - 1 - 2 * k >= 0)
        def _():
            pair_copy(h, k).wait_recv()

    def pg_copy(h, k):
        return pltpu.make_async_remote_copy(
            src_ref=pg_send.at[h, k],
            dst_ref=pg_recv.at[h, k],
            send_sem=pgs.at[h, k],
            recv_sem=pgr.at[h, k],
            device_id=where_is(partner),
            device_id_type=MESH,
        )

    def cg_copy(h, j):
        return pltpu.make_async_remote_copy(
            src_ref=c_send.at[h, j],
            dst_ref=c_recv.at[h, j],
            send_sem=cgs.at[h, j],
            recv_sem=cgr.at[h, j],
            device_id=where_is(down),
            device_id_type=MESH,
        )

    def pg_out(h, k):
        s = back - 1 - 2 * k
        at = pl.ds(s * rows, rows)
        pg_send[h, k, 0] = (acc_k[at, :] * scaling).astype(BF16)
        pg_send[h, k, 1] = acc_v[at, :].astype(BF16)

        @pl.when(me - 1 - 2 * k >= 0)
        def _():
            pg_copy(h, k).start()

    def keep_own(h, e):
        at = pl.ds((back - 2 * e) * rows, rows)
        own[h, e, 0] = acc_k[at, :] * scaling
        own[h, e, 1] = acc_v[at, :]

    def reduce_step(h, j):
        e = half - j

        @pl.when(me - 2 * e >= 0)
        def _():
            k = e - par

            @pl.when((k >= 0) & (k < half))
            def _():
                pg_copy(h, k).wait_recv()
                own[h, e] = own[h, e] + pg_recv[h, k].astype(F32)

            @pl.when(has_up & (j > 0))
            def _():
                cg_copy(h, j - 1).wait_recv()
                own[h, e] = own[h, e] + c_recv[h, j - 1].astype(F32)

    def reduce_send(h, j):
        @pl.when(me - 2 * (half - j) >= 0)
        def _():
            c_send[h, j] = own[h, half - j].astype(BF16)
            cg_copy(h, j).start()

    def finish(h):
        reduce_step(h, half)
        columns = pl.ds(pl.multiple_of(h * HEAD_SIZE, HEAD_SIZE), HEAD_SIZE)
        dk_ref[:, columns] = own[h, 0, 0].astype(BF16)
        dv_ref[:, columns] = own[h, 0, 1].astype(BF16)

    def compute(h, p):
        first = pl.multiple_of((h * GROUP + 2 * p) * HEAD_SIZE, HEAD_SIZE)
        second = pl.multiple_of(first + HEAD_SIZE, HEAD_SIZE)

        def two(ref):
            return jnp.concatenate(
                [ref[:, pl.ds(first, HEAD_SIZE)], ref[:, pl.ds(second, HEAD_SIZE)]], axis=0
            )

        q2, g2, o2 = two(q_ref), two(g_ref), two(o_ref)
        rd = jnp.sum((o2.astype(F32) * g2.astype(F32)).T, axis=0, keepdims=True)
        keys = kv[h, :, 0].reshape((back + 1) * rows, HEAD_SIZE)
        values = kv[h, :, 1].reshape((back + 1) * rows, HEAD_SIZE)
        st = lax.dot_general(keys, q2, NT, preferred_element_type=F32)
        dp = lax.dot_general(values, g2, NT, preferred_element_type=F32)
        key_at = lax.broadcasted_iota(jnp.int32, (rows, 2 * rows), 0)
        query_at = lax.rem(lax.broadcasted_iota(jnp.int32, (rows, 2 * rows), 1), rows)
        tri = key_at > query_at
        gone = [jnp.where(me - back + s < 0, 1e30, 0.0).astype(F32) for s in range(back)]

        def cut(a, s):
            return a[s * rows : (s + 1) * rows]

        c = scaling * math.log2(math.e)
        blocks = [jnp.where(tri, cut(st, 0) - gone[0], cut(st, back))]
        blocks += [cut(st, s) for s in range(1, back)]
        top = jnp.max(blocks[0], axis=0, keepdims=True)
        for s in range(1, back):
            top = jnp.maximum(top, jnp.max(blocks[s], axis=0, keepdims=True) - gone[s])
        top = top * c
        probs = [jnp.exp2(blocks[0] * c - top)]
        probs += [jnp.exp2(blocks[s] * c - (top + gone[s])) for s in range(1, back)]
        sums = jnp.sum(probs[0], axis=0, keepdims=True)
        for s in range(1, back):
            sums = sums + jnp.sum(probs[s], axis=0, keepdims=True)
        inv = 1.0 / sums
        dps = [jnp.where(tri, cut(dp, 0), cut(dp, back))] + [cut(dp, s) for s in range(1, back)]
        ws = [a * inv for a in probs]
        ds = [w * (a - rd) for w, a in zip(ws, dps)]

        def spread(parts):
            low = [jnp.where(tri, parts[0], 0.0)] + parts[1:] + [jnp.where(tri, 0.0, parts[0])]
            return jnp.concatenate([a.astype(BF16) for a in low], axis=0)

        wt, dst = spread(ws), spread(ds)
        acc_v[...] += jnp.dot(wt, g2, preferred_element_type=F32)
        acc_k[...] += jnp.dot(dst, q2, preferred_element_type=F32)
        dq = lax.dot_general(dst, keys, TN, preferred_element_type=F32) * scaling
        dq_ref[:, pl.ds(first, HEAD_SIZE)] = dq[:rows].astype(BF16)
        dq_ref[:, pl.ds(second, HEAD_SIZE)] = dq[rows:].astype(BF16)

    for h in range(heads):
        kv_loads[2 * h].wait()
        kv_loads[2 * h + 1].wait()
        send_own(h)

    def loop(count, fn):
        def body(i, carry):
            fn(i)
            return carry

        lax.fori_loop(0, count, body, 0)

    loop(half, lambda k: gather_step(0, k))
    for copy in loads:
        copy.wait()

    def per_head(h):
        loop(half, lambda k: gather_finish(h, k))
        acc_k[...] = jnp.zeros_like(acc_k)
        acc_v[...] = jnp.zeros_like(acc_v)

        def part(p):
            compute(h, p)

            @pl.when((h + 1 < heads) & (p < half))
            def _():
                gather_step(h + 1, p)

            @pl.when((h > 0) & (p < half))
            def _():
                reduce_step(h - 1, p)
                reduce_send(h - 1, p)

        loop(PAIRS, part)

        def rest(k):
            @pl.when(h + 1 < heads)
            def _():
                gather_step(h + 1, k)

            @pl.when(h > 0)
            def _():
                reduce_step(h - 1, k)
                reduce_send(h - 1, k)

        for k in range(PAIRS, half):
            rest(k)
        loop(half, lambda k: pg_out(h, k))
        loop(half + 1, lambda e: keep_own(h, e))

        @pl.when(h > 0)
        def _():
            finish(h - 1)

    loop(heads, per_head)

    def last(j):
        reduce_step(heads - 1, j)
        reduce_send(heads - 1, j)

    loop(half, last)
    finish(heads - 1)

    def drain(h):
        def inner(k):
            @pl.when(chain_out(k))
            def _():
                chain_copy(h, k).wait_send()

            @pl.when(pair_out(k))
            def _():
                pair_copy(h, k).wait_send()

            @pl.when(me - 1 - 2 * k >= 0)
            def _():
                pg_copy(h, k).wait_send()

            @pl.when(me - 2 * (half - k) >= 0)
            def _():
                cg_copy(h, k).wait_send()

        loop(half, inner)

    loop(heads, drain)


def local(query, key_input, value_input, output, out_grad):
    rows, width = query.shape
    blks, ulys = lax.axis_size("blk"), lax.axis_size("uly")
    back = WINDOW_KEYS // rows
    half = back // 2
    heads = KEY_VALUE_HEADS
    span = (back + 1) * rows
    pair = (2, rows, HEAD_SIZE)
    dma = pltpu.SemaphoreType.DMA
    any_spec = pl.BlockSpec(memory_space=pl.ANY)
    vmem_spec = pl.BlockSpec(memory_space=pltpu.VMEM)
    return pl.pallas_call(
        functools.partial(kernel, rows, back, blks, ulys),
        out_shape=(
            jax.ShapeDtypeStruct(query.shape, BF16),
            jax.ShapeDtypeStruct(key_input.shape, BF16),
            jax.ShapeDtypeStruct(value_input.shape, BF16),
        ),
        in_specs=[any_spec] * 5,
        out_specs=(vmem_spec,) * 3,
        scratch_shapes=[
            pltpu.VMEM((rows, width), BF16),
            pltpu.VMEM((rows, width), BF16),
            pltpu.VMEM((rows, width), BF16),
            pltpu.VMEM((heads, back + 1) + pair, BF16),
            pltpu.VMEM((span, HEAD_SIZE), F32),
            pltpu.VMEM((span, HEAD_SIZE), F32),
            pltpu.VMEM((heads, half + 1) + pair, F32),
            pltpu.VMEM((heads, half) + pair, BF16),
            pltpu.VMEM((heads, half) + pair, BF16),
            pltpu.VMEM((heads, half) + pair, BF16),
            pltpu.VMEM((heads, half) + pair, BF16),
            dma((3,)),
            dma((heads, 2)),
        ]
        + [dma((heads, half))] * 8,
        compiler_params=pltpu.CompilerParams(
            collective_id=0, has_side_effects=True, vmem_limit_bytes=60 * 1024 * 1024
        ),
    )(query, key_input, value_input, output, out_grad)


def solution(mesh):
    spec = P(("blk", "uly"), None)
    return jax.shard_map(
        local, mesh=mesh, in_specs=(spec,) * 5, out_specs=(spec,) * 3, check_vma=False
    )
```

```python
import functools
import math

import jax
import jax.numpy as jnp
from jax import lax
from jax.experimental import pallas as pl
from jax.experimental.pallas import tpu as pltpu
from jax.sharding import PartitionSpec as P

QUERY_HEADS = 32
KEY_VALUE_HEADS = 4
HEAD_SIZE = 128
WINDOW_KEYS = 1024
GROUP = QUERY_HEADS // KEY_VALUE_HEADS
PAIRS = GROUP // 2
MESH = pl.DeviceIdType.MESH
F32 = jnp.float32
BF16 = jnp.bfloat16
NT = (((1,), (1,)), ((), ()))
TN = (((0,), (0,)), ((), ()))


def kernel(
    rows, back, blks, ulys,
    q_hbm, k_hbm, v_hbm, o_hbm, g_hbm,
    dq_ref, dk_ref, dv_ref,
    q_ref, o_ref, g_ref, kv, acc_k, acc_v, own, pg_send, pg_recv, c_send, c_recv,
    load_sem, kv_sem, chain_ss, chain_rs, pair_ss, pair_rs, pgs, pgr, cgs, cgr,
):
    half = back // 2
    heads = KEY_VALUE_HEADS
    scaling = HEAD_SIZE ** (-0.5)
    total = blks * ulys
    me = lax.axis_index("blk") * ulys + lax.axis_index("uly")
    par = lax.rem(me, 2)
    partner = me + 1 - 2 * par
    up, down = me + 2, me - 2
    has_up, has_down = up < total, down >= 0

    def where_is(t):
        return (t // ulys, lax.rem(t, ulys))

    loads = [
        pltpu.make_async_copy(s, d, load_sem.at[i])
        for i, (s, d) in enumerate(((q_hbm, q_ref), (o_hbm, o_ref), (g_hbm, g_ref)))
    ]
    kv_loads = []
    for h in range(heads):
        for i, src in enumerate((k_hbm, v_hbm)):
            kv_loads.append(
                pltpu.make_async_copy(
                    src.at[:, h * HEAD_SIZE : (h + 1) * HEAD_SIZE], kv.at[h, back, i], kv_sem.at[h, i]
                )
            )
    for copy in kv_loads:
        copy.start()
    for copy in loads:
        copy.start()

    barrier = pltpu.get_barrier_semaphore()

    @pl.when(has_up)
    def _():
        pl.semaphore_signal(barrier, inc=1, device_id=where_is(up), device_id_type=MESH)

    @pl.when(has_down)
    def _():
        pl.semaphore_signal(barrier, inc=1, device_id=where_is(down), device_id_type=MESH)

    pl.semaphore_signal(barrier, inc=1, device_id=where_is(partner), device_id_type=MESH)
    pl.semaphore_wait(barrier, 1 + has_up.astype(jnp.int32) + has_down.astype(jnp.int32))

    def clear(s, carry):
        @pl.when(me - back + s < 0)
        def _():
            for h in range(heads):
                kv[h, s] = jnp.zeros((2, rows, HEAD_SIZE), BF16)

        return carry

    lax.fori_loop(0, back, clear, 0)

    def chain_copy(h, k):
        return pltpu.make_async_remote_copy(
            src_ref=kv.at[h, back - 2 * k],
            dst_ref=kv.at[h, back - 2 * k - 2],
            send_sem=chain_ss.at[h, k],
            recv_sem=chain_rs.at[h, k],
            device_id=where_is(up),
            device_id_type=MESH,
        )

    def pair_copy(h, k):
        return pltpu.make_async_remote_copy(
            src_ref=kv.at[h, back - 2 * k - 2 * par],
            dst_ref=kv.at[h, back - 1 - 2 * k],
            send_sem=pair_ss.at[h, k],
            recv_sem=pair_rs.at[h, k],
            device_id=where_is(partner),
            device_id_type=MESH,
        )

    def chain_out(k):
        return has_up & (me - 2 * k >= 0)

    def pair_out(k):
        return me - 2 * k - 2 * par >= 0

    def send_own(h):
        @pl.when(has_up)
        def _():
            chain_copy(h, 0).start()

        @pl.when(par == 0)
        def _():
            pair_copy(h, 0).start()

    def gather_step(h, k):
        @pl.when(me - 2 * k - 2 >= 0)
        def _():
            chain_copy(h, k).wait_recv()

            @pl.when(has_up & (k < half - 1))
            def _():
                chain_copy(h, k + 1).start()

            nxt = k + 1 - par

            @pl.when(nxt < half)
            def _():
                pair_copy(h, nxt).start()

    def gather_finish(h, k):
        @pl.when(me - 1 - 2 * k >= 0)
        def _():
            pair_copy(h, k).wait_recv()

    def pg_copy(h, k):
        return pltpu.make_async_remote_copy(
            src_ref=pg_send.at[h, k],
            dst_ref=pg_recv.at[h, k],
            send_sem=pgs.at[h, k],
            recv_sem=pgr.at[h, k],
            device_id=where_is(partner),
            device_id_type=MESH,
        )

    def cg_copy(h, j):
        return pltpu.make_async_remote_copy(
            src_ref=c_send.at[h, j],
            dst_ref=c_recv.at[h, j],
            send_sem=cgs.at[h, j],
            recv_sem=cgr.at[h, j],
            device_id=where_is(down),
            device_id_type=MESH,
        )

    def pg_out(h, k):
        s = back - 1 - 2 * k
        at = pl.ds(s * rows, rows)
        pg_send[h, k, 0] = (acc_k[at, :] * scaling).astype(BF16)
        pg_send[h, k, 1] = acc_v[at, :].astype(BF16)

        @pl.when(me - 1 - 2 * k >= 0)
        def _():
            pg_copy(h, k).start()

    def keep_own(h, e):
        at = pl.ds((back - 2 * e) * rows, rows)
        own[h, e, 0] = acc_k[at, :] * scaling
        own[h, e, 1] = acc_v[at, :]

    def reduce_step(h, j):
        e = half - j

        @pl.when(me - 2 * e >= 0)
        def _():
            k = e - par

            @pl.when((k >= 0) & (k < half))
            def _():
                pg_copy(h, k).wait_recv()
                own[h, e] = own[h, e] + pg_recv[h, k].astype(F32)

            @pl.when(has_up & (j > 0))
            def _():
                cg_copy(h, j - 1).wait_recv()
                own[h, e] = own[h, e] + c_recv[h, j - 1].astype(F32)

    def reduce_send(h, j):
        @pl.when(me - 2 * (half - j) >= 0)
        def _():
            c_send[h, j] = own[h, half - j].astype(BF16)
            cg_copy(h, j).start()

    def finish(h):
        reduce_step(h, half)
        columns = pl.ds(pl.multiple_of(h * HEAD_SIZE, HEAD_SIZE), HEAD_SIZE)
        dk_ref[:, columns] = own[h, 0, 0].astype(BF16)
        dv_ref[:, columns] = own[h, 0, 1].astype(BF16)

    def compute(h, p):
        first = pl.multiple_of((h * GROUP + 2 * p) * HEAD_SIZE, HEAD_SIZE)
        second = pl.multiple_of(first + HEAD_SIZE, HEAD_SIZE)

        def two(ref):
            return jnp.concatenate(
                [ref[:, pl.ds(first, HEAD_SIZE)], ref[:, pl.ds(second, HEAD_SIZE)]], axis=0
            )

        q2, g2, o2 = two(q_ref), two(g_ref), two(o_ref)
        rd = jnp.sum((o2.astype(F32) * g2.astype(F32)).T, axis=0, keepdims=True)
        keys = kv[h, :, 0].reshape((back + 1) * rows, HEAD_SIZE)
        values = kv[h, :, 1].reshape((back + 1) * rows, HEAD_SIZE)
        st = lax.dot_general(keys, q2, NT, preferred_element_type=F32)
        dp = lax.dot_general(values, g2, NT, preferred_element_type=F32)
        key_at = lax.broadcasted_iota(jnp.int32, (rows, 2 * rows), 0)
        query_at = lax.rem(lax.broadcasted_iota(jnp.int32, (rows, 2 * rows), 1), rows)
        tri = key_at > query_at
        gone = [jnp.where(me - back + s < 0, 1e30, 0.0).astype(F32) for s in range(back)]

        def cut(a, s):
            return a[s * rows : (s + 1) * rows]

        c = scaling * math.log2(math.e)
        blocks = [jnp.where(tri, cut(st, 0) - gone[0], cut(st, back))]
        blocks += [cut(st, s) for s in range(1, back)]
        top = jnp.max(blocks[0], axis=0, keepdims=True)
        for s in range(1, back):
            top = jnp.maximum(top, jnp.max(blocks[s], axis=0, keepdims=True) - gone[s])
        top = top * c
        probs = [jnp.exp2(blocks[0] * c - top)]
        probs += [jnp.exp2(blocks[s] * c - (top + gone[s])) for s in range(1, back)]
        sums = jnp.sum(probs[0], axis=0, keepdims=True)
        for s in range(1, back):
            sums = sums + jnp.sum(probs[s], axis=0, keepdims=True)
        inv = 1.0 / sums
        dps = [jnp.where(tri, cut(dp, 0), cut(dp, back))] + [cut(dp, s) for s in range(1, back)]
        ws = [a * inv for a in probs]
        ds = [w * (a - rd) for w, a in zip(ws, dps)]

        def spread(parts):
            low = [jnp.where(tri, parts[0], 0.0)] + parts[1:] + [jnp.where(tri, 0.0, parts[0])]
            return jnp.concatenate([a.astype(BF16) for a in low], axis=0)

        wt, dst = spread(ws), spread(ds)
        acc_v[...] += jnp.dot(wt, g2, preferred_element_type=F32)
        acc_k[...] += jnp.dot(dst, q2, preferred_element_type=F32)
        dq = lax.dot_general(dst, keys, TN, preferred_element_type=F32) * scaling
        dq_ref[:, pl.ds(first, HEAD_SIZE)] = dq[:rows].astype(BF16)
        dq_ref[:, pl.ds(second, HEAD_SIZE)] = dq[rows:].astype(BF16)

    for h in range(heads):
        kv_loads[2 * h].wait()
        kv_loads[2 * h + 1].wait()
        send_own(h)

    def loop(count, fn):
        def body(i, carry):
            fn(i)
            return carry

        lax.fori_loop(0, count, body, 0)

    def hop(k):
        loop(heads, lambda h: gather_step(h, k))

    loop(half - 1, hop)
    gather_step(0, half - 1)
    for copy in loads:
        copy.wait()

    def job(h, j):
        @pl.when((h >= 0) & (h < heads) & (j < half))
        def _():
            reduce_step(h, j)
            reduce_send(h, j)

        @pl.when((h >= 0) & (h < heads) & (j == half))
        def _():
            finish(h)

    lag = half + 1

    def per_head(h):
        @pl.when(h < heads)
        def _():
            loop(half, lambda k: gather_finish(h, k))
            acc_k[...] = jnp.zeros_like(acc_k)
            acc_v[...] = jnp.zeros_like(acc_v)

        def part(i):
            p = 2 * i

            @pl.when(h < heads)
            def _():
                compute(h, p)
                compute(h, p + 1)

            @pl.when((h == 0) & (p + 1 < heads))
            def _():
                gather_step(p + 1, half - 1)

            @pl.when((h == 0) & (p + 2 < heads))
            def _():
                gather_step(p + 2, half - 1)

        loop(PAIRS // 2, part)

        @pl.when(h < heads)
        def _():
            loop(half, lambda k: pg_out(h, k))
            loop(half + 1, lambda e: keep_own(h, e))

        for m in range(1, lag + 1):
            job(h - m, m - 1)

    loop(heads + lag, per_head)

    def drain(h):
        def inner(k):
            @pl.when(chain_out(k))
            def _():
                chain_copy(h, k).wait_send()

            @pl.when(pair_out(k))
            def _():
                pair_copy(h, k).wait_send()

            @pl.when(me - 1 - 2 * k >= 0)
            def _():
                pg_copy(h, k).wait_send()

            @pl.when(me - 2 * (half - k) >= 0)
            def _():
                cg_copy(h, k).wait_send()

        loop(half, inner)

    loop(heads, drain)


def local(query, key_input, value_input, output, out_grad):
    rows, width = query.shape
    blks, ulys = lax.axis_size("blk"), lax.axis_size("uly")
    back = WINDOW_KEYS // rows
    half = back // 2
    heads = KEY_VALUE_HEADS
    span = (back + 1) * rows
    pair = (2, rows, HEAD_SIZE)
    dma = pltpu.SemaphoreType.DMA
    any_spec = pl.BlockSpec(memory_space=pl.ANY)
    vmem_spec = pl.BlockSpec(memory_space=pltpu.VMEM)
    return pl.pallas_call(
        functools.partial(kernel, rows, back, blks, ulys),
        out_shape=(
            jax.ShapeDtypeStruct(query.shape, BF16),
            jax.ShapeDtypeStruct(key_input.shape, BF16),
            jax.ShapeDtypeStruct(value_input.shape, BF16),
        ),
        in_specs=[any_spec] * 5,
        out_specs=(vmem_spec,) * 3,
        scratch_shapes=[
            pltpu.VMEM((rows, width), BF16),
            pltpu.VMEM((rows, width), BF16),
            pltpu.VMEM((rows, width), BF16),
            pltpu.VMEM((heads, back + 1) + pair, BF16),
            pltpu.VMEM((span, HEAD_SIZE), F32),
            pltpu.VMEM((span, HEAD_SIZE), F32),
            pltpu.VMEM((heads, half + 1) + pair, F32),
            pltpu.VMEM((heads, half) + pair, BF16),
            pltpu.VMEM((heads, half) + pair, BF16),
            pltpu.VMEM((heads, half) + pair, BF16),
            pltpu.VMEM((heads, half) + pair, BF16),
            dma((3,)),
            dma((heads, 2)),
        ]
        + [dma((heads, half))] * 8,
        compiler_params=pltpu.CompilerParams(
            collective_id=0, has_side_effects=True, vmem_limit_bytes=60 * 1024 * 1024
        ),
    )(query, key_input, value_input, output, out_grad)


def solution(mesh):
    spec = P(("blk", "uly"), None)
    return jax.shard_map(
        local, mesh=mesh, in_specs=(spec,) * 5, out_specs=(spec,) * 3, check_vma=False
    )
```
